256 devices in a mesh: pipe: 2 (over core), dp: 64 (over y, x_hi, z), mp: 2 (over x_lo).
Axes of the slice: x: 4 (x_hi: 2, x_lo: 2; x = x_hi * 2 + x_lo), y: 4, z: 8, core: 2. Of those that a mesh axis runs over, the one named last changes fastest.
Arguments:
- token_ids: int32 [2, 32768], P('pipe', 'dp'), may hold values from 0 to 32127, as said below
- embedded: bfloat16 [2, 32768, 4096], P('pipe', 'dp', 'mp'), may hold values from -720 to 720
- norm_gain: float32 [2, 4096], P('pipe', 'mp'), may hold values from 0.25 to 1.75
- proj_grad: bfloat16 [2, 32768, 2048], P('pipe', 'dp'), may hold values from -6 to 6
- proj_weight: bfloat16 [2, 4096, 2048], P('pipe', 'mp'), may hold values from -0.125 to 0.125
- stream_grad: bfloat16 [2, 32768, 4096], P('pipe', 'dp', 'mp'), may hold values from -6 to 6
Outputs:
- table_grad: float32 [32128, 2, 2048], P('dp', 'mp', 'pipe')
The draws below stay inside these ranges and needn't reach their ends.
Inputs may be any that keep to these rules, and one draw needn't show every extreme that they name: `token_ids`: call block o the ids o * 502 to (o + 1) * 502 - 1. The 512 tokens of one stack on one index of dp hold at most 16 ids of any one block, and some block gets exactly 16 of them.
All inputs are finite; a program needn't handle non-finite values.
Results may differ from the reference program's by a relative error of at most 0.0029.
Values may be sent and summed in bfloat16 or wider, within the bound.
A program may use at most 128 MiB of HBM per device.

```python
import math
import jax
import jax.numpy as jnp
from jax import lax

D = 4096
VOCAB = 32128
INNER = 2048
TOK_DEV = 512
TOKENS = 32768
CAP = 16
VR = 502
N_DP = 64


def draw_token_ids(key, part):
    hot_rows = jax.random.randint(jax.random.fold_in(key, 7), (N_DP,), 0, VR)

    def draw_block(section_number, replica):
        full_owner = jax.random.randint(jax.random.fold_in(jax.random.fold_in(key, 11), section_number), (), 0, N_DP)
        block_key = jax.random.fold_in(jax.random.fold_in(key, 101 + section_number), replica)
        key_slots, key_order, key_choose, key_rows = jax.random.split(block_key, 4)
        remaining = jax.random.permutation(key_slots, (N_DP - 1) * CAP)[:TOK_DEV - CAP]
        owners_rest = (remaining // CAP + full_owner + 1) % N_DP
        owners = jnp.concatenate([jnp.full((CAP,), full_owner, jnp.int32), owners_rest.astype(jnp.int32)])
        owners = owners[jax.random.permutation(key_order, TOK_DEV)]
        chooser = jax.random.randint(key_choose, (TOK_DEV,), 0, 4)
        uniform_rows = jax.random.randint(key_rows, (TOK_DEV,), 0, VR)
        picked = jnp.where(chooser == 0, hot_rows[owners], uniform_rows)
        return (owners * VR + picked).astype(jnp.int32)
    sections = jnp.arange(2, dtype=jnp.int32)
    replicas = jnp.arange(N_DP, dtype=jnp.int32)
    blocks = jax.vmap(lambda section_number: jax.vmap(lambda replica: draw_block(section_number, replica))(replicas))(sections)
    return blocks.reshape(2, TOKENS)


def draw_embedded(key, part):
    key_base, key_rows = jax.random.split(key, 2)
    columns = jnp.arange(D, dtype=jnp.float32) / (D - 1)
    base = jax.random.normal(key_base, (2 * TOKENS, D), jnp.float32)
    row_scale = jnp.exp(jax.random.uniform(key_rows, (2 * TOKENS, 1), jnp.float32, 0.0, math.log(10.0)))
    column_scale = jnp.exp(columns * math.log(3.0))
    base = jnp.clip(base, -5.0, 5.0)
    return (base * row_scale * column_scale[None, :]).astype(jnp.bfloat16).reshape(2, TOKENS, D)


def steps_of(rng, extent, cuts, smallest, largest):
    def one(dim, shards_of):
        draws = jax.random.uniform(jax.random.fold_in(jax.random.fold_in(rng, 6), dim), (shards_of,), jnp.float32, smallest / len(cuts), largest / len(cuts))
        return jnp.repeat(jnp.exp(draws), extent[dim] // shards_of).reshape((-1,) + (1,) * (len(extent) - dim - 1))

    factor_of = one(*cuts[0])
    for cut in cuts[1:]:
        factor_of = factor_of * one(*cut)
    return factor_of


def noise(own_key, shape, deviation, limit, shards=(), held_as=jnp.bfloat16):
    drawn = jax.random.normal(own_key, shape, jnp.float32) * deviation
    if len(shards) > 0:
        drawn = steps_of(own_key, shape, shards, -0.22, 0.18) * drawn
    return jnp.clip(drawn, min=-limit, max=limit).astype(held_as)


def setup_inputs(seed: int = 0) -> dict:
    key_of = jax.random.split(jax.random.key(seed), 7)
    token_ids = draw_token_ids(jax.random.fold_in(key_of[6], 71), 0)
    embedded = draw_embedded(jax.random.fold_in(key_of[6], 71), 0)
    norm_gain = jnp.clip(1.0 + 0.15 * jax.random.normal(key_of[2], (2, D), jnp.float32), 0.25, 1.75)
    proj_grad = noise(key_of[3], (2, TOKENS, INNER), 1.0, 6.0, ((0, 2), (1, 64)))
    proj_weight = noise(key_of[4], (2, D, INNER), INNER ** -0.5, 0.125, ((0, 2), (1, 2)))
    stream_grad = noise(key_of[5], (2, TOKENS, D), 1.0, 6.0, ((0, 2), (1, 64), (2, 2)))
    return dict(token_ids=token_ids, embedded=embedded, norm_gain=norm_gain, proj_grad=proj_grad, proj_weight=proj_weight, stream_grad=stream_grad)


epsilon = 1e-06

def stack_back(grad, weight, embed, gain, stream):
    query_back = jnp.dot(grad, weight.T, preferred_element_type=jnp.float32)
    inputs = embed.astype(jnp.float32)
    scaled = query_back * gain.astype(jnp.float32)[None, :]
    square_sum = lax.optimization_barrier(jnp.sum(inputs * inputs, axis=1))
    mixed_sum = lax.optimization_barrier(jnp.sum(inputs * scaled, axis=1))
    inverse = lax.rsqrt(square_sum / D + epsilon)
    norm_back = inverse[:, None] * scaled - inputs * (inverse * inverse * inverse * mixed_sum / D)[:, None]
    return (stream.astype(jnp.float32) + norm_back).astype(jnp.bfloat16)

def reference(token_ids, embedded, norm_gain, proj_grad, proj_weight, stream_grad):
    first = stack_back(proj_grad[0], proj_weight[0], embedded[0], norm_gain[0], stream_grad[0])
    second = stack_back(proj_grad[1], proj_weight[1], embedded[1], norm_gain[1], stream_grad[1])
    all_rows = jnp.concatenate([first, second], axis=0).astype(jnp.float32)
    table = jax.ops.segment_sum(all_rows, token_ids.reshape(-1).astype(jnp.int32), num_segments=VOCAB)
    return table.reshape(VOCAB, 2, D // 2)
```

```python
import jax
import jax.numpy as jnp
from jax import lax
from jax.experimental import pallas as pl
from jax.experimental.pallas import tpu as pltpu
from jax.sharding import PartitionSpec as P

D = 4096
VOCAB = 32128
EPS = 1e-06

TOK = 512
CAP = 16
VR = 502
VP = 512
NDP = 64
INNER = 2048
FEAT = 2048
CF = 256
NB = FEAT // CF
NC = NB // 2
SLOTS = NDP * CAP
HALF = VR // 2
MESH = pl.DeviceIdType.MESH
NT = (((1,), (1,)), ((), ()))
F32 = jnp.float32
BF16 = jnp.bfloat16
I32 = jnp.int32


def placement(ids):
    block = lax.broadcasted_iota(I32, (NDP, TOK), 0)
    low = block * VR
    inside = jnp.logical_and(ids >= low, ids < low + VR)
    match = jnp.where(inside, 1.0, 0.0)
    before = jnp.where(
        lax.broadcasted_iota(I32, (TOK, TOK), 0) < lax.broadcasted_iota(I32, (TOK, TOK), 1), 1.0, 0.0
    ).astype(BF16)
    earlier = jnp.dot(match.astype(BF16), before, preferred_element_type=F32)
    slot = jnp.sum(match * (earlier + (block * CAP).astype(F32)), axis=0, keepdims=True).astype(I32)
    row = jnp.sum(match * (ids - low - HALF).astype(F32), axis=0, keepdims=True)
    placer = jnp.where(lax.broadcasted_iota(I32, (SLOTS, TOK), 0) == slot, 1.0, 0.0).astype(BF16)
    rows = lax.dot_general(
        placer, jnp.broadcast_to(row, (128, TOK)).astype(BF16), NT, preferred_element_type=F32
    )
    return placer, rows.astype(BF16).reshape(NDP, CAP, 128)


def kernel(
    ids_ref,
    gain_ref,
    emb_hbm,
    pg_hbm,
    w_hbm,
    st_hbm,
    out_hbm,
    pg,
    w,
    emb,
    st,
    scaled,
    square,
    mixed,
    inv,
    coef,
    sums_tx,
    sums_rx,
    ids_rx,
    place,
    rows_tx,
    rows_rx,
    send,
    recv,
    isend,
    irecv,
    onehot,
    table,
    in_sem,
    sum_sem,
    ids_sem,
    row_ssem,
    row_rsem,
    ssem,
    rsem,
    issem,
    irsem,
    osem,
):
    core = lax.axis_index("pipe")
    me = lax.axis_index("dp")
    half = lax.axis_index("mp")
    y, x, z = me // 16, (me // 8) % 2, me % 8

    def peer(q, k, dz):
        spot = (q + k) % 8
        return ((y + spot // 2) % 4) * 16 + ((x + spot) % 2) * 8 + (z + dz) % 8

    def to_peers(act):
        def step(q, carry):
            for k, dz in enumerate((0, 4, 3, 5, 2, 6, 1, 7)):
                if dz == 0:
                    @pl.when(q > 0)
                    def _():
                        act(peer(q, k, dz))
                else:
                    act(peer(q, k, dz))
            return carry

        lax.fori_loop(0, 8, step, 0)

    barrier = pltpu.get_barrier_semaphore()
    to_peers(lambda t: pl.semaphore_signal(barrier, inc=1, device_id={"dp": t}, device_id_type=MESH))
    pl.semaphore_signal(barrier, inc=1, device_id={"mp": 1 - half}, device_id_type=MESH)
    pl.semaphore_signal(barrier, inc=1, device_id={"pipe": 1 - core}, device_id_type=MESH)

    pg_in = pltpu.make_async_copy(pg_hbm.at[0], pg, in_sem.at[0])
    pg_in.start()

    def w_in(b):
        return pltpu.make_async_copy(w_hbm.at[0, pl.ds(b * CF, CF), :], w.at[b], in_sem.at[1 + b])

    def emb_in(b):
        return pltpu.make_async_copy(
            emb_hbm.at[0, :, pl.ds(b * CF, CF)], emb.at[b], in_sem.at[1 + NB + b]
        )

    def st_in(b):
        return pltpu.make_async_copy(
            st_hbm.at[0, :, pl.ds(b * CF, CF)], st.at[b], in_sem.at[1 + 2 * NB + b]
        )

    for b in range(NB):
        w_in(b).start()
        emb_in(b).start()
    for b in range(NB):
        st_in(b).start()

    placer, rows = placement(ids_ref[...])
    place[0] = placer
    isend[:, 0:CAP, :] = rows
    square[...] = jnp.zeros_like(square)
    mixed[...] = jnp.zeros_like(mixed)
    pg_in.wait()

    def project(b, carry):
        pltpu.make_async_copy(w_hbm.at[0, pl.ds(0, CF), :], w.at[b], in_sem.at[1 + b]).wait()
        pltpu.make_async_copy(
            emb_hbm.at[0, :, pl.ds(0, CF)], emb.at[b], in_sem.at[1 + NB + b]
        ).wait()
        s = lax.dot_general(pg[...], w[b], NT, preferred_element_type=F32) * gain_ref[b]
        scaled[b] = s
        e = emb[b].astype(F32)
        ee, es = e * e, e * s
        square[...] += ee[:, :128] + ee[:, 128:]
        mixed[...] += es[:, :128] + es[:, 128:]
        return carry

    lax.fori_loop(0, NB, project, 0)

    sums_tx[0:1] = jnp.sum(square[...].T, axis=0, keepdims=True)
    sums_tx[1:2] = jnp.sum(mixed[...].T, axis=0, keepdims=True)
    for b in range(NB):
        st_in(b).wait()
    pl.semaphore_wait(barrier, NDP - 1 + 2)

    sums_copy = pltpu.make_async_remote_copy(
        src_ref=sums_tx,
        dst_ref=sums_rx,
        send_sem=sum_sem.at[0],
        recv_sem=sum_sem.at[1],
        device_id={"mp": 1 - half},
        device_id_type=MESH,
    )
    ids_copy = pltpu.make_async_remote_copy(
        src_ref=ids_ref,
        dst_ref=ids_rx,
        send_sem=ids_sem.at[0],
        recv_sem=ids_sem.at[1],
        device_id={"pipe": 1 - core},
        device_id_type=MESH,
    )
    ids_copy.start()
    sums_copy.start()

    ids_copy.wait()
    placer, rows = placement(ids_rx[...])
    place[1] = placer
    isend[:, CAP : 2 * CAP, :] = rows

    sums_copy.wait()
    total = sums_tx[...] + sums_rx[...]
    inverse = lax.rsqrt(total[0:1] / D + EPS)
    factor = inverse * inverse * inverse * total[1:2] / D
    inv[...] = jnp.broadcast_to(inverse, (128, TOK)).T
    coef[...] = jnp.broadcast_to(factor, (128, TOK)).T

    def finished(b):
        def lanes(i):
            cut = slice(i * 128, (i + 1) * 128)
            back = inv[...] * scaled[b, :, cut] - emb[b, :, cut].astype(F32) * coef[...]
            return (st[b, :, cut].astype(F32) + back).astype(BF16)

        return jnp.concatenate([lanes(i) for i in range(CF // 128)], axis=1)

    def swap(c):
        return pltpu.make_async_remote_copy(
            src_ref=rows_tx.at[c],
            dst_ref=rows_rx.at[c],
            send_sem=row_ssem.at[c],
            recv_sem=row_rsem.at[c],
            device_id={"pipe": 1 - core},
            device_id_type=MESH,
        )

    def out_copy(src, dst, s, r, t):
        return pltpu.make_async_remote_copy(
            src_ref=src.at[t],
            dst_ref=dst.at[me],
            send_sem=s,
            recv_sem=r,
            device_id={"dp": t},
            device_id_type=MESH,
        )

    to_peers(lambda t: out_copy(isend, irecv, issem, irsem, t).start())
    irecv[me] = isend[me]

    for c in range(NC):
        rows_tx[c] = finished((1 - core) * NC + c)
        swap(c).start()
        send[c, :, 0:CAP, :] = (
            jnp.dot(place[0], finished(core * NC + c), preferred_element_type=F32)
            .astype(BF16)
            .reshape(NDP, CAP, CF)
        )
        swap(c).wait()
        send[c, :, CAP : 2 * CAP, :] = (
            jnp.dot(place[1], rows_rx[c], preferred_element_type=F32)
            .astype(BF16)
            .reshape(NDP, CAP, CF)
        )
        recv[c, me] = send[c, me]
        to_peers(lambda t: out_copy(send.at[c], recv.at[c], ssem.at[c], rsem.at[c], t).start())

    def all_but_one(ref, sem):
        part = ref.at[pl.ds(0, NDP - 1)]
        pltpu.make_async_copy(part, part, sem).wait()

    all_but_one(irecv, irsem)
    index = irecv[...].astype(F32).reshape(2 * SLOTS, 128).T[0:1].astype(I32) + HALF
    onehot[...] = jnp.where(lax.broadcasted_iota(I32, (VP, 2 * SLOTS), 0) == index, 1.0, 0.0).astype(BF16)

    def put(c):
        return pltpu.make_async_copy(
            table.at[c], out_hbm.at[:, pl.ds(c * CF, CF)], osem.at[c]
        )

    for c in range(NC):
        all_but_one(recv.at[c], rsem.at[c])
        sums = jnp.dot(
            onehot[...], recv[c].reshape(2 * SLOTS, CF), preferred_element_type=F32
        )
        table[c] = sums[:VR]
        put(c).start()
    all_but_one(isend, issem)
    for c in range(NC):
        all_but_one(send.at[c], ssem.at[c])
        put(c).wait()


def on_device(token_ids, embedded, norm_gain, proj_grad, proj_weight, stream_grad):
    anywhere = pl.BlockSpec(memory_space=pl.ANY)
    vmem = pl.BlockSpec(memory_space=pltpu.VMEM)
    dma = pltpu.SemaphoreType.DMA
    table = pl.pallas_call(
        kernel,
        out_shape=jax.ShapeDtypeStruct((VR, FEAT // 2), F32),
        in_specs=[vmem, vmem] + [anywhere] * 4,
        out_specs=anywhere,
        scratch_shapes=[
            pltpu.VMEM((TOK, INNER), BF16),
            pltpu.VMEM((NB, CF, INNER), BF16),
            pltpu.VMEM((NB, TOK, CF), BF16),
            pltpu.VMEM((NB, TOK, CF), BF16),
            pltpu.VMEM((NB, TOK, CF), F32),
            pltpu.VMEM((TOK, 128), F32),
            pltpu.VMEM((TOK, 128), F32),
            pltpu.VMEM((TOK, 128), F32),
            pltpu.VMEM((TOK, 128), F32),
            pltpu.VMEM((2, TOK), F32),
            pltpu.VMEM((2, TOK), F32),
            pltpu.VMEM((1, TOK), I32),
            pltpu.VMEM((2, SLOTS, TOK), BF16),
            pltpu.VMEM((NC, TOK, CF), BF16),
            pltpu.VMEM((NC, TOK, CF), BF16),
            pltpu.VMEM((NC, NDP, 2 * CAP, CF), BF16),
            pltpu.VMEM((NC, NDP, 2 * CAP, CF), BF16),
            pltpu.VMEM((NDP, 2 * CAP, 128), BF16),
            pltpu.VMEM((NDP, 2 * CAP, 128), BF16),
            pltpu.VMEM((VP, 2 * SLOTS), BF16),
            pltpu.VMEM((NC, VR, CF), F32),
            dma((1 + 3 * NB,)),
            dma((2,)),
            dma((2,)),
            dma((NC,)),
            dma((NC,)),
            dma((NC,)),
            dma((NC,)),
            dma,
            dma,
            dma((NC,)),
        ],
        compiler_params=pltpu.CompilerParams(
            collective_id=0, has_side_effects=True, vmem_limit_bytes=58 * 1024 * 1024
        ),
    )(
        token_ids,
        norm_gain.reshape(NB, 1, CF),
        embedded,
        proj_grad,
        proj_weight,
        stream_grad,
    )
    return table.reshape(VR, 1, FEAT // 2)


def solution(mesh):
    return jax.shard_map(
        on_device,
        mesh=mesh,
        in_specs=(
            P("pipe", "dp"),
            P("pipe", "dp", "mp"),
            P("pipe", "mp"),
            P("pipe", "dp", None),
            P("pipe", "mp", None),
            P("pipe", "dp", "mp"),
        ),
        out_specs=P("dp", "mp", "pipe"),
        check_vma=False,
    )
```

```python
import jax
import jax.numpy as jnp
from jax import lax
from jax.experimental import pallas as pl
from jax.experimental.pallas import tpu as pltpu
from jax.sharding import PartitionSpec as P

D = 4096
VOCAB = 32128
EPS = 1e-06

TOK = 512
CAP = 16
VR = 502
VP = 504
NDP = 64
INNER = 2048
FEAT = 2048
CF = 128
BF = 256
NB = FEAT // BF
NF = FEAT // CF
NC = NF // 2
SLOTS = NDP * CAP
ROWS = 2 * SLOTS
HALF = VR // 2
GROUP = 8 * 2 * CAP
MOVES = (2, 1, 0, 0, 0, 0, -1, -2)
REMOTE = NDP - 4
MESH = pl.DeviceIdType.MESH
NT = (((1,), (1,)), ((), ()))
F32 = jnp.float32
BF16 = jnp.bfloat16
I32 = jnp.int32


def placement(ids, first):
    block = lax.broadcasted_iota(I32, (NDP, TOK), 0)
    low = block * VR
    inside = jnp.logical_and(ids >= low, ids < low + VR)
    match = jnp.where(inside, 1.0, 0.0)
    before = jnp.where(
        lax.broadcasted_iota(I32, (TOK, TOK), 0) < lax.broadcasted_iota(I32, (TOK, TOK), 1), 1.0, 0.0
    ).astype(BF16)
    earlier = match * jnp.dot(match.astype(BF16), before, preferred_element_type=F32)
    rank = jnp.sum(earlier, axis=0, keepdims=True).astype(I32)
    slot = jnp.sum(earlier + match * (block * CAP).astype(F32), axis=0, keepdims=True).astype(I32)
    placer = jnp.where(lax.broadcasted_iota(I32, (SLOTS, TOK), 0) == slot, 1.0, 0.0).astype(BF16)
    ranks = jnp.where(lax.broadcasted_iota(I32, (128, TOK), 0) == rank + first, 1.0, 0.0).astype(BF16)
    rows = (match * (ids - low - HALF).astype(F32)).astype(BF16)
    return placer, lax.dot_general(rows, ranks, NT, preferred_element_type=F32)


def kernel(
    ids_ref,
    gain_ref,
    emb_hbm,
    pg_hbm,
    w_hbm,
    st_hbm,
    out_hbm,
    pg,
    w,
    emb,
    st,
    scaled,
    square,
    mixed,
    inv,
    coef,
    sums_tx,
    sums_rx,
    ids_rx,
    place,
    rows_tx,
    rows_rx,
    send,
    recv,
    isend,
    irecv,
    onehot,
    far_tx,
    far_rx,
    near_tx,
    near_rx,
    back_tx,
    back_rx,
    table,
    in_sem,
    sum_sem,
    ids_sem,
    row_ssem,
    row_rsem,
    ssem,
    rsem,
    issem,
    irsem,
    tab_ssem,
    tab_rsem,
    osem,
):
    core = lax.axis_index("pipe")
    me = lax.axis_index("dp")
    half = lax.axis_index("mp")
    y, x, z = me // 16, (me // 8) % 2, me % 8
    here = me // 8

    def column(spot):
        return ((y + spot // 2) % 4) * 16 + ((x + spot) % 2) * 8

    def plane(dz):
        return (z + dz + 8) % 8

    def signal(where):
        pl.semaphore_signal(barrier, inc=1, device_id=where, device_id_type=MESH)

    barrier = pltpu.get_barrier_semaphore()
    signal({"mp": 1 - half})
    signal({"pipe": 1 - core})

    def greet(spot, carry):
        for dz in (-2, -1, 1, 2):
            signal({"dp": column(spot) + plane(dz)})

        @pl.when(spot > 0)
        def _():
            signal({"dp": column(spot) + z})

        return carry

    lax.fori_loop(0, 8, greet, 0)

    def in_copy(src, dst, i):
        return pltpu.make_async_copy(src, dst, in_sem.at[i])

    def w_in(b):
        return in_copy(w_hbm.at[0, pl.ds(b * BF, BF), :], w.at[b], 1 + b)

    def emb_in(f):
        return in_copy(emb_hbm.at[0, :, pl.ds(f * CF, CF)], emb.at[f], 1 + NB + f)

    def st_in(f):
        return in_copy(st_hbm.at[0, :, pl.ds(f * CF, CF)], st.at[f], 1 + NB + NF + f)

    pg_in = in_copy(pg_hbm.at[0], pg, 0)
    pg_in.start()
    for b in range(NB):
        w_in(b).start()
        emb_in(2 * b).start()
        emb_in(2 * b + 1).start()
    for f in range(NF):
        st_in(f).start()

    place[0], own_rows = placement(ids_ref[...], 0)
    square[...] = jnp.zeros_like(square)
    mixed[...] = jnp.zeros_like(mixed)

    ids_copy = pltpu.make_async_remote_copy(
        src_ref=ids_ref,
        dst_ref=ids_rx,
        send_sem=ids_sem.at[0],
        recv_sem=ids_sem.at[1],
        device_id={"pipe": 1 - core},
        device_id_type=MESH,
    )
    pl.semaphore_wait(barrier, 41)
    ids_copy.start()
    pg_in.wait()

    def project(b, carry):
        in_copy(w_hbm.at[0, pl.ds(0, BF), :], w.at[b], 1 + b).wait()
        s = lax.dot_general(pg[...], w[b], NT, preferred_element_type=F32) * gain_ref[b]
        for i in range(2):
            f = 2 * b + i
            in_copy(emb_hbm.at[0, :, pl.ds(0, CF)], emb.at[f], 1 + NB + f).wait()
            part = s[:, i * CF : (i + 1) * CF]
            scaled[f] = part
            e = emb[f].astype(F32)
            square[...] += e * e
            mixed[...] += e * part
        return carry

    lax.fori_loop(0, NB, project, 0)

    sums_tx[0:1] = jnp.sum(square[...].T, axis=0, keepdims=True)
    sums_tx[1:2] = jnp.sum(mixed[...].T, axis=0, keepdims=True)

    sums_copy = pltpu.make_async_remote_copy(
        src_ref=sums_tx,
        dst_ref=sums_rx,
        send_sem=sum_sem.at[0],
        recv_sem=sum_sem.at[1],
        device_id={"mp": 1 - half},
        device_id_type=MESH,
    )
    ids_copy.wait()
    sums_copy.start()
    place[1], other_rows = placement(ids_rx[...], CAP)
    isend[...] = (own_rows + other_rows).reshape(NDP, 1, 128)
    for f in range(NF):
        st_in(f).wait()

    def send_blocks(src, dst, s_sem, r_sem, s):
        def step(q, carry):
            for i in (0, 7, 2, 1, 6, 3, 5, 4):
                spot = (q + i) % 8
                owner = column(spot) + plane(s * (4 - i))

                def start(spot=spot, owner=owner, i=i):
                    pltpu.make_async_remote_copy(
                        src_ref=src.at[owner],
                        dst_ref=dst.at[i * 8 + here],
                        send_sem=s_sem,
                        recv_sem=r_sem,
                        device_id={"dp": column(spot) + plane(s * MOVES[i])},
                        device_id_type=MESH,
                    ).start()

                if MOVES[i] == 0:
                    pl.when(spot != 0)(start)
                else:
                    start()
            return carry

        lax.fori_loop(0, 8, step, 0)
        for i in range(8):
            if MOVES[i] == 0:
                dst[i * 8 + here] = src[here * 8 + plane(s * (4 - i))]

    def await_blocks(ref, sem):
        part = ref.at[pl.ds(0, REMOTE)]
        pltpu.make_async_copy(part, part, sem).wait()

    for kind in range(2):
        send_blocks(isend, irecv.at[kind], issem.at[kind], irsem.at[kind], 1 - 2 * kind)

    sums_copy.wait()
    total = sums_tx[...] + sums_rx[...]
    inverse = lax.rsqrt(total[0:1] / D + EPS)
    factor = inverse * inverse * inverse * total[1:2] / D
    inv[...] = jnp.broadcast_to(inverse, (128, TOK)).T
    coef[...] = jnp.broadcast_to(factor, (128, TOK)).T

    def finished(f):
        back = inv[...] * scaled[f] - emb[f].astype(F32) * coef[...]
        return (st[f].astype(F32) + back).astype(BF16)

    def swap(c):
        return pltpu.make_async_remote_copy(
            src_ref=rows_tx.at[c],
            dst_ref=rows_rx.at[c],
            send_sem=row_ssem.at[c],
            recv_sem=row_rsem.at[c],
            device_id={"pipe": 1 - core},
            device_id_type=MESH,
        )

    def hand_over(c):
        rows_tx[c] = finished((1 - core) * NC + c)
        swap(c).start()

    def direction(c):
        return 1 - 2 * (c % 2)

    def spread(c):
        def slots(i, rows):
            send[c, :, i * CAP : (i + 1) * CAP, :] = (
                jnp.dot(place[i], rows, preferred_element_type=F32).astype(BF16).reshape(NDP, CAP, CF)
            )

        slots(0, finished(core * NC + c))
        swap(c).wait()
        slots(1, rows_rx[c])
        send_blocks(send.at[c], recv.at[c], ssem.at[c], rsem.at[c], direction(c))

    def summed(c, first, groups):
        rows = recv[c, first * 8 : (first + groups) * 8].reshape(groups * GROUP, CF)
        picks = onehot[c % 2, :, first * GROUP : (first + groups) * GROUP]
        return jnp.dot(picks, rows, preferred_element_type=F32)

    def pass_on(src, dst, c, i, s):
        return pltpu.make_async_remote_copy(
            src_ref=src.at[c],
            dst_ref=dst.at[c],
            send_sem=tab_ssem.at[i, c],
            recv_sem=tab_rsem.at[i, c],
            device_id={"dp": here * 8 + plane(s)},
            device_id_type=MESH,
        )

    def far(c):
        return pass_on(far_tx, far_rx, c, 0, direction(c))

    def near(c):
        return pass_on(near_tx, near_rx, c, 1, direction(c))

    def back(c):
        return pass_on(back_tx, back_rx, c, 2, -direction(c))

    def put(c):
        return pltpu.make_async_copy(table.at[c], out_hbm.at[:, :, pl.ds(c * CF, CF)], osem.at[c])

    def first_sums(c):
        await_blocks(recv.at[c], rsem.at[c])
        far_tx[c] = summed(c, 0, 3).astype(BF16)
        far(c).start()
        back_tx[c] = summed(c, 5, 3).astype(BF16)
        back(c).start()

    def second_sums(c):
        own = summed(c, 3, 1)
        far(c).wait()
        near_tx[c] = (own + far_rx[c].astype(F32)).astype(BF16)
        near(c).start()

    def last_sums(c):
        own = summed(c, 4, 1)
        back(c).wait()
        own = own + back_rx[c].astype(F32)
        near(c).wait()
        own = own + near_rx[c].astype(F32)
        table[c] = own[:VR].reshape(VR, 1, CF)
        put(c).start()

    AHEAD = 2
    for c in range(AHEAD):
        hand_over(c)
    for c in range(AHEAD):
        spread(c)

    slot = lax.broadcasted_iota(I32, (NDP, ROWS), 1)
    unfold = jnp.where(slot // (2 * CAP) == lax.broadcasted_iota(I32, (NDP, ROWS), 0), 1.0, 0.0).astype(BF16)
    lane = lax.broadcasted_iota(I32, (2 * CAP, ROWS), 1) % (2 * CAP)
    take = lane == lax.broadcasted_iota(I32, (2 * CAP, ROWS), 0)
    for kind in range(2):
        await_blocks(irecv.at[kind], irsem.at[kind])
        got = irecv[kind].reshape(NDP, 128).T[: 2 * CAP].astype(BF16)
        spots = jnp.dot(got, unfold, preferred_element_type=F32)
        index = jnp.sum(jnp.where(take, spots, 0.0), axis=0, keepdims=True).astype(I32) + HALF
        onehot[kind] = jnp.where(lax.broadcasted_iota(I32, (VP, ROWS), 0) == index, 1.0, 0.0).astype(BF16)

    for c in range(NC + 2):
        if c + AHEAD < NC:
            hand_over(c + AHEAD)
        if c < NC:
            first_sums(c)
        if c + AHEAD < NC:
            spread(c + AHEAD)
        if 0 <= c - 1 < NC:
            second_sums(c - 1)
        if 0 <= c - 2 < NC:
            last_sums(c - 2)

    for kind in range(2):
        await_blocks(isend, issem.at[kind])
    for c in range(NC):
        await_blocks(send.at[c], ssem.at[c])
        put(c).wait()


def on_device(token_ids, embedded, norm_gain, proj_grad, proj_weight, stream_grad):
    anywhere = pl.BlockSpec(memory_space=pl.ANY)
    vmem = pl.BlockSpec(memory_space=pltpu.VMEM)
    dma = pltpu.SemaphoreType.DMA
    return pl.pallas_call(
        kernel,
        out_shape=jax.ShapeDtypeStruct((VR, 1, FEAT // 2), F32),
        in_specs=[vmem, vmem] + [anywhere] * 4,
        out_specs=anywhere,
        scratch_shapes=[
            pltpu.VMEM((TOK, INNER), BF16),
            pltpu.VMEM((NB, BF, INNER), BF16),
            pltpu.VMEM((NF, TOK, CF), BF16),
            pltpu.VMEM((NF, TOK, CF), BF16),
            pltpu.VMEM((NF, TOK, CF), F32),
            pltpu.VMEM((TOK, 128), F32),
            pltpu.VMEM((TOK, 128), F32),
            pltpu.VMEM((TOK, 128), F32),
            pltpu.VMEM((TOK, 128), F32),
            pltpu.VMEM((2, TOK), F32),
            pltpu.VMEM((2, TOK), F32),
            pltpu.VMEM((1, TOK), I32),
            pltpu.VMEM((2, SLOTS, TOK), BF16),
            pltpu.VMEM((NC, TOK, CF), BF16),
            pltpu.VMEM((NC, TOK, CF), BF16),
            pltpu.VMEM((NC, NDP, 2 * CAP, CF), BF16),
            pltpu.VMEM((NC, NDP, 2 * CAP, CF), BF16),
            pltpu.VMEM((NDP, 1, 128), F32),
            pltpu.VMEM((2, NDP, 1, 128), F32),
            pltpu.VMEM((2, VP, ROWS), BF16),
            pltpu.VMEM((NC, VP, CF), BF16),
            pltpu.VMEM((NC, VP, CF), BF16),
            pltpu.VMEM((NC, VP, CF), BF16),
            pltpu.VMEM((NC, VP, CF), BF16),
            pltpu.VMEM((NC, VP, CF), BF16),
            pltpu.VMEM((NC, VP, CF), BF16),
            pltpu.VMEM((NC, VR, 1, CF), F32),
            dma((1 + NB + 2 * NF,)),
            dma((2,)),
            dma((2,)),
            dma((NC,)),
            dma((NC,)),
            dma((NC,)),
            dma((NC,)),
            dma((2,)),
            dma((2,)),
            dma((3, NC)),
            dma((3, NC)),
            dma((NC,)),
        ],
        compiler_params=pltpu.CompilerParams(
            collective_id=0, has_side_effects=True, vmem_limit_bytes=58 * 1024 * 1024
        ),
    )(
        token_ids,
        norm_gain.reshape(NB, 1, BF),
        embedded,
        proj_grad,
        proj_weight,
        stream_grad,
    )


def solution(mesh):
    return jax.shard_map(
        on_device,
        mesh=mesh,
        in_specs=(
            P("pipe", "dp"),
            P("pipe", "dp", "mp"),
            P("pipe", "mp"),
            P("pipe", "dp", None),
            P("pipe", "mp", None),
            P("pipe", "dp", "mp"),
        ),
        out_specs=P("dp", "mp", "pipe"),
        check_vma=False,
    )
```

```python
import jax
import jax.numpy as jnp
from jax import lax
from jax.experimental import pallas as pl
from jax.experimental.pallas import tpu as pltpu
from jax.sharding import PartitionSpec as P

D = 4096
VOCAB = 32128
EPS = 1e-06

TOK = 512
CAP = 16
VR = 502
VP = 504
NDP = 64
INNER = 2048
FEAT = 2048
CF = 128
BF = 256
NB = FEAT // BF
NF = FEAT // CF
NC = NF // 2
AHEAD = 4
SLOTS = NDP * CAP
ROWS = 2 * SLOTS
HALF = VR // 2
GROUP = 8 * 2 * CAP
MOVES = (2, 1, 0, 0, 0, 0, -1, -2)
REMOTE = NDP - 4
MESH = pl.DeviceIdType.MESH
NT = (((1,), (1,)), ((), ()))
F32 = jnp.float32
BF16 = jnp.bfloat16
I32 = jnp.int32


def placement(ids, first):
    block = lax.broadcasted_iota(I32, (NDP, TOK), 0)
    low = block * VR
    inside = jnp.logical_and(ids >= low, ids < low + VR)
    match = jnp.where(inside, 1.0, 0.0)
    before = jnp.where(
        lax.broadcasted_iota(I32, (TOK, TOK), 0) < lax.broadcasted_iota(I32, (TOK, TOK), 1), 1.0, 0.0
    ).astype(BF16)
    earlier = match * jnp.dot(match.astype(BF16), before, preferred_element_type=F32)
    rank = jnp.sum(earlier, axis=0, keepdims=True).astype(I32)
    slot = jnp.sum(earlier + match * (block * CAP).astype(F32), axis=0, keepdims=True).astype(I32)
    placer = jnp.where(lax.broadcasted_iota(I32, (SLOTS, TOK), 0) == slot, 1.0, 0.0).astype(BF16)
    ranks = jnp.where(lax.broadcasted_iota(I32, (128, TOK), 0) == rank + first, 1.0, 0.0).astype(BF16)
    rows = (match * (ids - low - HALF).astype(F32)).astype(BF16)
    return placer, lax.dot_general(rows, ranks, NT, preferred_element_type=F32)


def kernel(
    ids_ref,
    gain_ref,
    emb_hbm,
    pg_hbm,
    w_hbm,
    st_hbm,
    table,
    pg,
    w,
    emb,
    st,
    scaled,
    square,
    mixed,
    inv,
    coef,
    sums_tx,
    sums_rx,
    ids_rx,
    place,
    rows_tx,
    rows_rx,
    send,
    recv,
    isend,
    irecv,
    onehot,
    far_tx,
    far_rx,
    near_tx,
    near_rx,
    back_tx,
    back_rx,
    in_sem,
    sum_sem,
    ids_sem,
    row_ssem,
    row_rsem,
    ssem,
    rsem,
    issem,
    irsem,
    tab_ssem,
    tab_rsem,
):
    core = lax.axis_index("pipe")
    me = lax.axis_index("dp")
    half = lax.axis_index("mp")
    y, x, z = me // 16, (me // 8) % 2, me % 8
    here = me // 8

    def column(spot):
        return ((y + spot // 2) % 4) * 16 + ((x + spot) % 2) * 8

    def plane(dz):
        return (z + dz + 8) % 8

    def signal(where):
        pl.semaphore_signal(barrier, inc=1, device_id=where, device_id_type=MESH)

    barrier = pltpu.get_barrier_semaphore()
    signal({"mp": 1 - half})
    signal({"pipe": 1 - core})

    def greet(spot, carry):
        for dz in (-2, -1, 1, 2):
            signal({"dp": column(spot) + plane(dz)})

        @pl.when(spot > 0)
        def _():
            signal({"dp": column(spot) + z})

        return carry

    lax.fori_loop(0, 8, greet, 0)

    def in_copy(src, dst, i):
        return pltpu.make_async_copy(src, dst, in_sem.at[i])

    def w_in(b):
        return in_copy(w_hbm.at[0, pl.ds(b * BF, BF), :], w.at[b], 1 + b)

    def emb_in(f):
        return in_copy(emb_hbm.at[0, :, pl.ds(f * CF, CF)], emb.at[f], 1 + NB + f)

    def st_in(f):
        return in_copy(st_hbm.at[0, :, pl.ds(f * CF, CF)], st.at[f], 1 + NB + NF + f)

    pg_in = in_copy(pg_hbm.at[0], pg, 0)
    pg_in.start()
    for b in range(NB):
        w_in(b).start()
        emb_in(2 * b).start()
        emb_in(2 * b + 1).start()
    for f in range(NF):
        st_in(f).start()

    place[0], own_rows = placement(ids_ref[...], 0)
    square[...] = jnp.zeros_like(square)
    mixed[...] = jnp.zeros_like(mixed)

    ids_copy = pltpu.make_async_remote_copy(
        src_ref=ids_ref,
        dst_ref=ids_rx,
        send_sem=ids_sem.at[0],
        recv_sem=ids_sem.at[1],
        device_id={"pipe": 1 - core},
        device_id_type=MESH,
    )
    pg_in.wait()

    def project(b, carry):
        in_copy(w_hbm.at[0, pl.ds(0, BF), :], w.at[b], 1 + b).wait()
        s = lax.dot_general(pg[...], w[b], NT, preferred_element_type=F32) * gain_ref[b]
        for i in range(2):
            f = 2 * b + i
            in_copy(emb_hbm.at[0, :, pl.ds(0, CF)], emb.at[f], 1 + NB + f).wait()
            part = s[:, i * CF : (i + 1) * CF]
            scaled[f] = part
            e = emb[f].astype(F32)
            square[...] += e * e
            mixed[...] += e * part
        return carry

    lax.fori_loop(0, NB, project, 0)

    sums_tx[0:1] = jnp.sum(square[...].T, axis=0, keepdims=True)
    sums_tx[1:2] = jnp.sum(mixed[...].T, axis=0, keepdims=True)

    sums_copy = pltpu.make_async_remote_copy(
        src_ref=sums_tx,
        dst_ref=sums_rx,
        send_sem=sum_sem.at[0],
        recv_sem=sum_sem.at[1],
        device_id={"mp": 1 - half},
        device_id_type=MESH,
    )
    pl.semaphore_wait(barrier, 41)
    ids_copy.start()
    sums_copy.start()
    ids_copy.wait()
    place[1], other_rows = placement(ids_rx[...], CAP)
    isend[...] = (own_rows + other_rows).reshape(NDP, 1, 128)
    for f in range(NF):
        st_in(f).wait()

    def send_blocks(src, dst, s_sem, r_sem, s):
        def step(q, carry):
            for i in (0, 7, 2, 1, 6, 3, 5, 4):
                spot = (q + i) % 8
                owner = column(spot) + plane(s * (4 - i))

                def start(spot=spot, owner=owner, i=i):
                    pltpu.make_async_remote_copy(
                        src_ref=src.at[owner],
                        dst_ref=dst.at[i * 8 + here],
                        send_sem=s_sem,
                        recv_sem=r_sem,
                        device_id={"dp": column(spot) + plane(s * MOVES[i])},
                        device_id_type=MESH,
                    ).start()

                if MOVES[i] == 0:
                    pl.when(spot != 0)(start)
                else:
                    start()
            return carry

        lax.fori_loop(0, 8, step, 0)
        for i in range(8):
            if MOVES[i] == 0:
                dst[i * 8 + here] = src[here * 8 + plane(s * (4 - i))]

    def await_blocks(ref, sem):
        part = ref.at[pl.ds(0, REMOTE)]
        pltpu.make_async_copy(part, part, sem).wait()

    sums_copy.wait()
    total = sums_tx[...] + sums_rx[...]
    inverse = lax.rsqrt(total[0:1] / D + EPS)
    factor = inverse * inverse * inverse * total[1:2] / D
    inv[...] = jnp.broadcast_to(inverse, (128, TOK)).T
    coef[...] = jnp.broadcast_to(factor, (128, TOK)).T

    def finished(f):
        back = inv[...] * scaled[f] - emb[f].astype(F32) * coef[...]
        return (st[f].astype(F32) + back).astype(BF16)

    def swap(c):
        return pltpu.make_async_remote_copy(
            src_ref=rows_tx.at[c],
            dst_ref=rows_rx.at[c],
            send_sem=row_ssem.at[c],
            recv_sem=row_rsem.at[c],
            device_id={"pipe": 1 - core},
            device_id_type=MESH,
        )

    def hand_over(c):
        rows_tx[c] = finished((1 - core) * NC + c)
        swap(c).start()

    def direction(c):
        return 1 - 2 * (c % 2)

    def spread(c):
        def slots(i, rows):
            send[c, :, i * CAP : (i + 1) * CAP, :] = (
                jnp.dot(place[i], rows, preferred_element_type=F32).astype(BF16).reshape(NDP, CAP, CF)
            )

        slots(0, finished(core * NC + c))
        swap(c).wait()
        slots(1, rows_rx[c])
        send_blocks(send.at[c], recv.at[c], ssem.at[c], rsem.at[c], direction(c))

    def summed(c, first, groups):
        rows = recv[c, first * 8 : (first + groups) * 8].reshape(groups * GROUP, CF)
        picks = onehot[c % 2, :, first * GROUP : (first + groups) * GROUP]
        return jnp.dot(picks, rows, preferred_element_type=F32)

    def pass_on(src, dst, c, i, s):
        return pltpu.make_async_remote_copy(
            src_ref=src.at[c],
            dst_ref=dst.at[c],
            send_sem=tab_ssem.at[i, c],
            recv_sem=tab_rsem.at[i, c],
            device_id={"dp": here * 8 + plane(s)},
            device_id_type=MESH,
        )

    def far(c):
        return pass_on(far_tx, far_rx, c, 0, direction(c))

    def near(c):
        return pass_on(near_tx, near_rx, c, 1, direction(c))

    def back(c):
        return pass_on(back_tx, back_rx, c, 2, -direction(c))

    def first_sums(c):
        await_blocks(recv.at[c], rsem.at[c])
        far_tx[c] = summed(c, 0, 3).astype(BF16)
        far(c).start()
        back_tx[c] = summed(c, 5, 3).astype(BF16)
        back(c).start()

    def second_sums(c):
        own = summed(c, 3, 1)
        far(c).wait()
        near_tx[c] = (own + far_rx[c].astype(F32)).astype(BF16)
        near(c).start()

    def last_sums(c):
        own = summed(c, 4, 1)
        back(c).wait()
        own = own + back_rx[c].astype(F32)
        near(c).wait()
        own = own + near_rx[c].astype(F32)
        table[:, :, c * CF : (c + 1) * CF] = own[:VR].reshape(VR, 1, CF)

    hand_over(0)
    hand_over(1)
    spread(0)
    for kind in range(2):
        send_blocks(isend, irecv.at[kind], issem.at[kind], irsem.at[kind], 1 - 2 * kind)
    for c in range(1, AHEAD):
        hand_over(c + 1)
        spread(c)

    slot = lax.broadcasted_iota(I32, (NDP, ROWS), 1)
    unfold = jnp.where(slot // (2 * CAP) == lax.broadcasted_iota(I32, (NDP, ROWS), 0), 1.0, 0.0).astype(BF16)
    lane = lax.broadcasted_iota(I32, (2 * CAP, ROWS), 1) % (2 * CAP)
    take = lane == lax.broadcasted_iota(I32, (2 * CAP, ROWS), 0)
    for kind in range(2):
        await_blocks(irecv.at[kind], irsem.at[kind])
        got = irecv[kind].reshape(NDP, 128).T[: 2 * CAP].astype(BF16)
        spots = jnp.dot(got, unfold, preferred_element_type=F32)
        index = jnp.sum(jnp.where(take, spots, 0.0), axis=0, keepdims=True).astype(I32) + HALF
        onehot[kind] = jnp.where(lax.broadcasted_iota(I32, (VP, ROWS), 0) == index, 1.0, 0.0).astype(BF16)

    for c in range(NC + 2):
        if c + AHEAD + 1 < NC:
            hand_over(c + AHEAD + 1)
        if c < NC:
            first_sums(c)
        if c + AHEAD < NC:
            spread(c + AHEAD)
        if 0 <= c - 1 < NC:
            second_sums(c - 1)
        if 0 <= c - 2 < NC:
            last_sums(c - 2)

    for kind in range(2):
        await_blocks(isend, issem.at[kind])
    for c in range(NC):
        await_blocks(send.at[c], ssem.at[c])


def on_device(token_ids, embedded, norm_gain, proj_grad, proj_weight, stream_grad):
    anywhere = pl.BlockSpec(memory_space=pl.ANY)
    vmem = pl.BlockSpec(memory_space=pltpu.VMEM)
    dma = pltpu.SemaphoreType.DMA
    table = pl.pallas_call(
        kernel,
        out_shape=pltpu.VMEM((VR, 1, FEAT // 2), F32),
        in_specs=[vmem, vmem] + [anywhere] * 4,
        out_specs=vmem,
        scratch_shapes=[
            pltpu.VMEM((TOK, INNER), BF16),
            pltpu.VMEM((NB, BF, INNER), BF16),
            pltpu.VMEM((NF, TOK, CF), BF16),
            pltpu.VMEM((NF, TOK, CF), BF16),
            pltpu.VMEM((NF, TOK, CF), F32),
            pltpu.VMEM((TOK, 128), F32),
            pltpu.VMEM((TOK, 128), F32),
            pltpu.VMEM((TOK, 128), F32),
            pltpu.VMEM((TOK, 128), F32),
            pltpu.VMEM((2, TOK), F32),
            pltpu.VMEM((2, TOK), F32),
            pltpu.VMEM((1, TOK), I32),
            pltpu.VMEM((2, SLOTS, TOK), BF16),
            pltpu.VMEM((NC, TOK, CF), BF16),
            pltpu.VMEM((NC, TOK, CF), BF16),
            pltpu.VMEM((NC, NDP, 2 * CAP, CF), BF16),
            pltpu.VMEM((NC, NDP, 2 * CAP, CF), BF16),
            pltpu.VMEM((NDP, 1, 128), F32),
            pltpu.VMEM((2, NDP, 1, 128), F32),
            pltpu.VMEM((2, VP, ROWS), BF16),
            pltpu.VMEM((NC, VP, CF), BF16),
            pltpu.VMEM((NC, VP, CF), BF16),
            pltpu.VMEM((NC, VP, CF), BF16),
            pltpu.VMEM((NC, VP, CF), BF16),
            pltpu.VMEM((NC, VP, CF), BF16),
            pltpu.VMEM((NC, VP, CF), BF16),
            dma((1 + NB + 2 * NF,)),
            dma((2,)),
            dma((2,)),
            dma((NC,)),
            dma((NC,)),
            dma((NC,)),
            dma((NC,)),
            dma((2,)),
            dma((2,)),
            dma((3, NC)),
            dma((3, NC)),
        ],
        compiler_params=pltpu.CompilerParams(
            collective_id=0, has_side_effects=True, vmem_limit_bytes=56 * 1024 * 1024
        ),
    )(
        token_ids,
        norm_gain.reshape(NB, 1, BF),
        embedded,
        proj_grad,
        proj_weight,
        stream_grad,
    )
    return table


def solution(mesh):
    return jax.shard_map(
        on_device,
        mesh=mesh,
        in_specs=(
            P("pipe", "dp"),
            P("pipe", "dp", "mp"),
            P("pipe", "mp"),
            P("pipe", "dp", None),
            P("pipe", "mp", None),
            P("pipe", "dp", "mp"),
        ),
        out_specs=P("dp", "mp", "pipe"),
        check_vma=False,
    )
```

```python
import jax
import jax.numpy as jnp
from jax import lax
from jax.experimental import pallas as pl
from jax.experimental.pallas import tpu as pltpu
from jax.sharding import PartitionSpec as P

D = 4096
VOCAB = 32128
EPS = 1e-06

TOK = 512
CAP = 16
VR = 502
VP = 504
NDP = 64
INNER = 2048
FEAT = 2048
CF = 128
BF = 512
NB = FEAT // BF
NF = FEAT // CF
NC = NF // 2
AHEAD = 4
SLOTS = NDP * CAP
ROWS = 2 * SLOTS
HALF = VR // 2
GROUP = 8 * 2 * CAP
MOVES = (2, 1, 0, 0, 0, 0, -1, -2)
REMOTE = NDP - 4
MESH = pl.DeviceIdType.MESH
NT = (((1,), (1,)), ((), ()))
F32 = jnp.float32
BF16 = jnp.bfloat16
I32 = jnp.int32


def placement(ids, first):
    block = lax.broadcasted_iota(I32, (NDP, TOK), 0)
    low = block * VR
    inside = jnp.logical_and(ids >= low, ids < low + VR)
    match = jnp.where(inside, 1.0, 0.0)
    before = jnp.where(
        lax.broadcasted_iota(I32, (TOK, TOK), 0) < lax.broadcasted_iota(I32, (TOK, TOK), 1), 1.0, 0.0
    ).astype(BF16)
    earlier = match * jnp.dot(match.astype(BF16), before, preferred_element_type=F32)
    rank = jnp.sum(earlier, axis=0, keepdims=True).astype(I32)
    slot = jnp.sum(earlier + match * (block * CAP).astype(F32), axis=0, keepdims=True).astype(I32)
    placer = jnp.where(lax.broadcasted_iota(I32, (SLOTS, TOK), 0) == slot, 1.0, 0.0).astype(BF16)
    ranks = jnp.where(lax.broadcasted_iota(I32, (128, TOK), 0) == rank + first, 1.0, 0.0).astype(BF16)
    rows = (match * (ids - low - HALF).astype(F32)).astype(BF16)
    return placer, lax.dot_general(rows, ranks, NT, preferred_element_type=F32)


def kernel(
    ids_ref,
    gain_ref,
    emb_hbm,
    pg_hbm,
    w_hbm,
    st_hbm,
    table,
    pg,
    w,
    emb,
    st,
    scaled,
    square,
    mixed,
    inv,
    coef,
    sums_tx,
    sums_rx,
    ids_rx,
    place,
    rows_tx,
    rows_rx,
    send,
    recv,
    isend,
    irecv,
    onehot,
    far_tx,
    far_rx,
    near_tx,
    near_rx,
    back_tx,
    back_rx,
    in_sem,
    sum_sem,
    ids_sem,
    row_ssem,
    row_rsem,
    ssem,
    rsem,
    issem,
    irsem,
    tab_ssem,
    tab_rsem,
):
    core = lax.axis_index("pipe")
    me = lax.axis_index("dp")
    half = lax.axis_index("mp")
    y, x, z = me // 16, (me // 8) % 2, me % 8
    here = me // 8

    def column(spot):
        return ((y + spot // 2) % 4) * 16 + ((x + spot) % 2) * 8

    def plane(dz):
        return (z + dz + 8) % 8

    def signal(where):
        pl.semaphore_signal(barrier, inc=1, device_id=where, device_id_type=MESH)

    barrier = pltpu.get_barrier_semaphore()
    signal({"mp": 1 - half})
    signal({"pipe": 1 - core})

    def greet(spot, carry):
        for dz in (-2, -1, 1, 2):
            signal({"dp": column(spot) + plane(dz)})

        @pl.when(spot > 0)
        def _():
            signal({"dp": column(spot) + z})

        return carry

    lax.fori_loop(0, 8, greet, 0)

    def in_copy(src, dst, i):
        return pltpu.make_async_copy(src, dst, in_sem.at[i])

    def w_in(b):
        return in_copy(w_hbm.at[0, pl.ds(b * BF, BF), :], w.at[b], 1 + b)

    def emb_in(f):
        return in_copy(emb_hbm.at[0, :, pl.ds(f * CF, CF)], emb.at[f], 1 + NB + f)

    def st_in(f):
        return in_copy(st_hbm.at[0, :, pl.ds(f * CF, CF)], st.at[f], 1 + NB + NF + f)

    pg_in = in_copy(pg_hbm.at[0], pg, 0)
    pg_in.start()
    for b in range(NB):
        w_in(b).start()
        for f in range(BF // CF * b, BF // CF * (b + 1)):
            emb_in(f).start()
    for f in range(NF):
        st_in(f).start()

    place[0], own_rows = placement(ids_ref[...], 0)
    square[...] = jnp.zeros_like(square)
    mixed[...] = jnp.zeros_like(mixed)

    ids_copy = pltpu.make_async_remote_copy(
        src_ref=ids_ref,
        dst_ref=ids_rx,
        send_sem=ids_sem.at[0],
        recv_sem=ids_sem.at[1],
        device_id={"pipe": 1 - core},
        device_id_type=MESH,
    )
    pg_in.wait()

    def project(b, carry):
        in_copy(w_hbm.at[0, pl.ds(0, BF), :], w.at[b], 1 + b).wait()
        s = lax.dot_general(pg[...], w[b], NT, preferred_element_type=F32) * gain_ref[b]
        for i in range(BF // CF):
            f = BF // CF * b + i
            in_copy(emb_hbm.at[0, :, pl.ds(0, CF)], emb.at[f], 1 + NB + f).wait()
            part = s[:, i * CF : (i + 1) * CF]
            scaled[f] = part
            e = emb[f].astype(F32)
            square[...] += e * e
            mixed[...] += e * part
        return carry

    lax.fori_loop(0, NB, project, 0)

    sums_tx[0:1] = jnp.sum(square[...].T, axis=0, keepdims=True)
    sums_tx[1:2] = jnp.sum(mixed[...].T, axis=0, keepdims=True)

    sums_copy = pltpu.make_async_remote_copy(
        src_ref=sums_tx,
        dst_ref=sums_rx,
        send_sem=sum_sem.at[0],
        recv_sem=sum_sem.at[1],
        device_id={"mp": 1 - half},
        device_id_type=MESH,
    )
    pl.semaphore_wait(barrier, 41)
    ids_copy.start()
    sums_copy.start()
    ids_copy.wait()
    place[1], other_rows = placement(ids_rx[...], CAP)
    isend[...] = (own_rows + other_rows).reshape(NDP, 1, 128)
    for f in range(NF):
        st_in(f).wait()

    def send_blocks(src, dst, s_sem, r_sem, s):
        def step(q, carry):
            for i in (0, 7, 2, 1, 6, 3, 5, 4):
                spot = (q + i) % 8
                owner = column(spot) + plane(s * (4 - i))

                def start(spot=spot, owner=owner, i=i):
                    pltpu.make_async_remote_copy(
                        src_ref=src.at[owner],
                        dst_ref=dst.at[i * 8 + here],
                        send_sem=s_sem,
                        recv_sem=r_sem,
                        device_id={"dp": column(spot) + plane(s * MOVES[i])},
                        device_id_type=MESH,
                    ).start()

                if MOVES[i] == 0:
                    pl.when(spot != 0)(start)
                else:
                    start()
            return carry

        lax.fori_loop(0, 8, step, 0)
        for i in range(8):
            if MOVES[i] == 0:
                dst[i * 8 + here] = src[here * 8 + plane(s * (4 - i))]

    def await_blocks(ref, sem):
        part = ref.at[pl.ds(0, REMOTE)]
        pltpu.make_async_copy(part, part, sem).wait()

    sums_copy.wait()
    total = sums_tx[...] + sums_rx[...]
    inverse = lax.rsqrt(total[0:1] / D + EPS)
    factor = inverse * inverse * inverse * total[1:2] / D
    inv[...] = jnp.broadcast_to(inverse, (128, TOK)).T
    coef[...] = jnp.broadcast_to(factor, (128, TOK)).T

    def finished(f):
        back = inv[...] * scaled[f] - emb[f].astype(F32) * coef[...]
        return (st[f].astype(F32) + back).astype(BF16)

    def swap(c):
        return pltpu.make_async_remote_copy(
            src_ref=rows_tx.at[c],
            dst_ref=rows_rx.at[c],
            send_sem=row_ssem.at[c],
            recv_sem=row_rsem.at[c],
            device_id={"pipe": 1 - core},
            device_id_type=MESH,
        )

    def hand_over(c):
        rows_tx[c] = finished((1 - core) * NC + c)
        swap(c).start()

    def direction(c):
        return 1 - 2 * (c % 2)

    def spread(c):
        def slots(i, rows):
            send[c, :, i * CAP : (i + 1) * CAP, :] = (
                jnp.dot(place[i], rows, preferred_element_type=F32).astype(BF16).reshape(NDP, CAP, CF)
            )

        slots(0, finished(core * NC + c))
        swap(c).wait()
        slots(1, rows_rx[c])
        send_blocks(send.at[c], recv.at[c], ssem.at[c], rsem.at[c], direction(c))

    def summed(c, first, groups):
        rows = recv[c, first * 8 : (first + groups) * 8].reshape(groups * GROUP, CF)
        picks = onehot[c % 2, :, first * GROUP : (first + groups) * GROUP]
        return jnp.dot(picks, rows, preferred_element_type=F32)

    def pass_on(src, dst, c, i, s):
        return pltpu.make_async_remote_copy(
            src_ref=src.at[c],
            dst_ref=dst.at[c],
            send_sem=tab_ssem.at[i, c],
            recv_sem=tab_rsem.at[i, c],
            device_id={"dp": here * 8 + plane(s)},
            device_id_type=MESH,
        )

    def far(c):
        return pass_on(far_tx, far_rx, c, 0, direction(c))

    def near(c):
        return pass_on(near_tx, near_rx, c, 1, direction(c))

    def back(c):
        return pass_on(back_tx, back_rx, c, 2, -direction(c))

    def first_sums(c):
        await_blocks(recv.at[c], rsem.at[c])
        far_tx[c] = summed(c, 0, 3).astype(BF16)
        far(c).start()
        back_tx[c] = summed(c, 5, 3).astype(BF16)
        back(c).start()

    def second_sums(c):
        own = summed(c, 3, 1)
        far(c).wait_recv()
        near_tx[c] = (own + far_rx[c].astype(F32)).astype(BF16)
        near(c).start()

    def last_sums(c):
        own = summed(c, 4, 1)
        back(c).wait_recv()
        own = own + back_rx[c].astype(F32)
        near(c).wait_recv()
        own = own + near_rx[c].astype(F32)
        table[:, :, c * CF : (c + 1) * CF] = own[:VR].reshape(VR, 1, CF)

    hand_over(0)
    hand_over(1)
    spread(0)
    for kind in range(2):
        send_blocks(isend, irecv.at[kind], issem.at[kind], irsem.at[kind], 1 - 2 * kind)
    for c in range(1, AHEAD):
        hand_over(c + 1)
        spread(c)

    slot = lax.broadcasted_iota(I32, (NDP, ROWS), 1)
    unfold = jnp.where(slot // (2 * CAP) == lax.broadcasted_iota(I32, (NDP, ROWS), 0), 1.0, 0.0).astype(BF16)
    lane = lax.broadcasted_iota(I32, (2 * CAP, ROWS), 1) % (2 * CAP)
    take = lane == lax.broadcasted_iota(I32, (2 * CAP, ROWS), 0)
    for kind in range(2):
        await_blocks(irecv.at[kind], irsem.at[kind])
        got = irecv[kind].reshape(NDP, 128).T[: 2 * CAP].astype(BF16)
        spots = jnp.dot(got, unfold, preferred_element_type=F32)
        index = jnp.sum(jnp.where(take, spots, 0.0), axis=0, keepdims=True).astype(I32) + HALF
        onehot[kind] = jnp.where(lax.broadcasted_iota(I32, (VP, ROWS), 0) == index, 1.0, 0.0).astype(BF16)

    for c in range(NC + 2):
        if c + AHEAD + 1 < NC:
            hand_over(c + AHEAD + 1)
        if c < NC:
            first_sums(c)
        if c + AHEAD < NC:
            spread(c + AHEAD)
        if 0 <= c - 1 < NC:
            second_sums(c - 1)
        if 0 <= c - 2 < NC:
            last_sums(c - 2)

    for kind in range(2):
        await_blocks(isend, issem.at[kind])
    for c in range(NC):
        await_blocks(send.at[c], ssem.at[c])
        for copy in (far(c), near(c), back(c)):
            copy.wait_send()


def on_device(token_ids, embedded, norm_gain, proj_grad, proj_weight, stream_grad):
    anywhere = pl.BlockSpec(memory_space=pl.ANY)
    vmem = pl.BlockSpec(memory_space=pltpu.VMEM)
    dma = pltpu.SemaphoreType.DMA
    table = pl.pallas_call(
        kernel,
        out_shape=pltpu.VMEM((VR, 1, FEAT // 2), F32),
        in_specs=[vmem, vmem] + [anywhere] * 4,
        out_specs=vmem,
        scratch_shapes=[
            pltpu.VMEM((TOK, INNER), BF16),
            pltpu.VMEM((NB, BF, INNER), BF16),
            pltpu.VMEM((NF, TOK, CF), BF16),
            pltpu.VMEM((NF, TOK, CF), BF16),
            pltpu.VMEM((NF, TOK, CF), F32),
            pltpu.VMEM((TOK, 128), F32),
            pltpu.VMEM((TOK, 128), F32),
            pltpu.VMEM((TOK, 128), F32),
            pltpu.VMEM((TOK, 128), F32),
            pltpu.VMEM((2, TOK), F32),
            pltpu.VMEM((2, TOK), F32),
            pltpu.VMEM((1, TOK), I32),
            pltpu.VMEM((2, SLOTS, TOK), BF16),
            pltpu.VMEM((NC, TOK, CF), BF16),
            pltpu.VMEM((NC, TOK, CF), BF16),
            pltpu.VMEM((NC, NDP, 2 * CAP, CF), BF16),
            pltpu.VMEM((NC, NDP, 2 * CAP, CF), BF16),
            pltpu.VMEM((NDP, 1, 128), F32),
            pltpu.VMEM((2, NDP, 1, 128), F32),
            pltpu.VMEM((2, VP, ROWS), BF16),
            pltpu.VMEM((NC, VP, CF), BF16),
            pltpu.VMEM((NC, VP, CF), BF16),
            pltpu.VMEM((NC, VP, CF), BF16),
            pltpu.VMEM((NC, VP, CF), BF16),
            pltpu.VMEM((NC, VP, CF), BF16),
            pltpu.VMEM((NC, VP, CF), BF16),
            dma((1 + NB + 2 * NF,)),
            dma((2,)),
            dma((2,)),
            dma((NC,)),
            dma((NC,)),
            dma((NC,)),
            dma((NC,)),
            dma((2,)),
            dma((2,)),
            dma((3, NC)),
            dma((3, NC)),
        ],
        compiler_params=pltpu.CompilerParams(
            collective_id=0, has_side_effects=True, vmem_limit_bytes=56 * 1024 * 1024
        ),
    )(
        token_ids,
        norm_gain.reshape(NB, 1, BF),
        embedded,
        proj_grad,
        proj_weight,
        stream_grad,
    )
    return table


def solution(mesh):
    return jax.shard_map(
        on_device,
        mesh=mesh,
        in_specs=(
            P("pipe", "dp"),
            P("pipe", "dp", "mp"),
            P("pipe", "mp"),
            P("pipe", "dp", None),
            P("pipe", "mp", None),
            P("pipe", "dp", "mp"),
        ),
        out_specs=P("dp", "mp", "pipe"),
        check_vma=False,
    )
```

```python
import jax
import jax.numpy as jnp
from jax import lax
from jax.experimental import pallas as pl
from jax.experimental.pallas import tpu as pltpu
from jax.sharding import PartitionSpec as P

D = 4096
VOCAB = 32128
EPS = 1e-06

TOK = 512
CAP = 16
VR = 502
VP = 504
NDP = 64
INNER = 2048
FEAT = 2048
CF = 128
BF = 512
NB = FEAT // BF
NF = FEAT // CF
NC = NF // 2
AHEAD = 4
SLOTS = NDP * CAP
ROWS = 2 * SLOTS
HALF = VR // 2
GROUP = 8 * 2 * CAP
MOVES = (2, 1, 0, 0, 0, 0, -1, -2)
REMOTE = NDP - 4
MESH = pl.DeviceIdType.MESH
NT = (((1,), (1,)), ((), ()))
F32 = jnp.float32
BF16 = jnp.bfloat16
I32 = jnp.int32


def placement(ids, first):
    block = lax.broadcasted_iota(I32, (NDP, TOK), 0)
    low = block * VR
    inside = jnp.logical_and(ids >= low, ids < low + VR)
    match = jnp.where(inside, 1.0, 0.0)
    before = jnp.where(
        lax.broadcasted_iota(I32, (TOK, TOK), 0) < lax.broadcasted_iota(I32, (TOK, TOK), 1), 1.0, 0.0
    ).astype(BF16)
    earlier = match * jnp.dot(match.astype(BF16), before, preferred_element_type=F32)
    rank = jnp.sum(earlier, axis=0, keepdims=True).astype(I32)
    slot = jnp.sum(earlier + match * (block * CAP).astype(F32), axis=0, keepdims=True).astype(I32)
    placer = jnp.where(lax.broadcasted_iota(I32, (SLOTS, TOK), 0) == slot, 1.0, 0.0).astype(BF16)
    ranks = jnp.where(lax.broadcasted_iota(I32, (128, TOK), 0) == rank + first, 1.0, 0.0).astype(BF16)
    rows = (match * (ids - low - HALF).astype(F32)).astype(BF16)
    return placer, lax.dot_general(rows, ranks, NT, preferred_element_type=F32)


def kernel(
    ids_ref,
    gain_ref,
    emb_hbm,
    pg_hbm,
    w_hbm,
    st_hbm,
    table,
    pg,
    w,
    emb,
    st,
    scaled,
    square,
    mixed,
    inv,
    coef,
    sums_tx,
    sums_rx,
    ids_rx,
    place,
    rows_tx,
    rows_rx,
    send,
    recv,
    isend,
    irecv,
    onehot,
    far_tx,
    far_rx,
    near_tx,
    near_rx,
    back_tx,
    back_rx,
    in_sem,
    sum_sem,
    ids_sem,
    row_ssem,
    row_rsem,
    ssem,
    rsem,
    issem,
    irsem,
    tab_ssem,
    tab_rsem,
):
    core = lax.axis_index("pipe")
    me = lax.axis_index("dp")
    half = lax.axis_index("mp")
    y, x, z = me // 16, (me // 8) % 2, me % 8
    here = me // 8

    def column(spot):
        return ((y + spot // 2) % 4) * 16 + ((x + spot) % 2) * 8

    def plane(dz):
        return (z + dz + 8) % 8

    def signal(where):
        pl.semaphore_signal(barrier, inc=1, device_id=where, device_id_type=MESH)

    barrier = pltpu.get_barrier_semaphore()
    signal({"mp": 1 - half})
    signal({"pipe": 1 - core})

    def greet(spot, carry):
        for dz in (-2, -1, 1, 2):
            signal({"dp": column(spot) + plane(dz)})

        @pl.when(spot > 0)
        def _():
            signal({"dp": column(spot) + z})

        return carry

    lax.fori_loop(0, 8, greet, 0)

    def in_copy(src, dst, i):
        return pltpu.make_async_copy(src, dst, in_sem.at[i])

    def w_in(b):
        return in_copy(w_hbm.at[0, pl.ds(b * BF, BF), :], w.at[b], 1 + b)

    def emb_in(f):
        return in_copy(emb_hbm.at[0, :, pl.ds(f * CF, CF)], emb.at[f], 1 + NB + f)

    def st_in(f):
        return in_copy(st_hbm.at[0, :, pl.ds(f * CF, CF)], st.at[f], 1 + NB + NF + f)

    pg_in = in_copy(pg_hbm.at[0], pg, 0)
    pg_in.start()
    for b in range(NB):
        w_in(b).start()
        for f in range(BF // CF * b, BF // CF * (b + 1)):
            emb_in(f).start()
    for f in range(NF):
        st_in(f).start()

    place[0], own_rows = placement(ids_ref[...], 0)
    square[...] = jnp.zeros_like(square)
    mixed[...] = jnp.zeros_like(mixed)

    ids_copy = pltpu.make_async_remote_copy(
        src_ref=ids_ref,
        dst_ref=ids_rx,
        send_sem=ids_sem.at[0],
        recv_sem=ids_sem.at[1],
        device_id={"pipe": 1 - core},
        device_id_type=MESH,
    )
    pg_in.wait()

    def project(b, carry):
        in_copy(w_hbm.at[0, pl.ds(0, BF), :], w.at[b], 1 + b).wait()
        s = lax.dot_general(pg[...], w[b], NT, preferred_element_type=F32) * gain_ref[b]
        for i in range(BF // CF):
            f = BF // CF * b + i
            in_copy(emb_hbm.at[0, :, pl.ds(0, CF)], emb.at[f], 1 + NB + f).wait()
            part = s[:, i * CF : (i + 1) * CF]
            scaled[f] = part
            e = emb[f].astype(F32)
            square[...] += e * e
            mixed[...] += e * part
        return carry

    lax.fori_loop(0, NB, project, 0)

    sums_tx[0:1] = jnp.sum(square[...].T, axis=0, keepdims=True)
    sums_tx[1:2] = jnp.sum(mixed[...].T, axis=0, keepdims=True)

    sums_copy = pltpu.make_async_remote_copy(
        src_ref=sums_tx,
        dst_ref=sums_rx,
        send_sem=sum_sem.at[0],
        recv_sem=sum_sem.at[1],
        device_id={"mp": 1 - half},
        device_id_type=MESH,
    )
    pl.semaphore_wait(barrier, 41)
    ids_copy.start()
    sums_copy.start()
    ids_copy.wait()
    place[1], other_rows = placement(ids_rx[...], CAP)
    isend[...] = (own_rows + other_rows).reshape(NDP, 1, 128)
    for f in range(NF):
        st_in(f).wait()

    def send_blocks(src, dst, s_sem, r_sem, s):
        def step(q, carry):
            for i in (0, 7, 2, 1, 6, 3, 5, 4):
                spot = (q + i) % 8
                owner = column(spot) + plane(s * (4 - i))

                def start(spot=spot, owner=owner, i=i):
                    pltpu.make_async_remote_copy(
                        src_ref=src.at[owner],
                        dst_ref=dst.at[i * 8 + here],
                        send_sem=s_sem,
                        recv_sem=r_sem,
                        device_id={"dp": column(spot) + plane(s * MOVES[i])},
                        device_id_type=MESH,
                    ).start()

                if MOVES[i] == 0:
                    pl.when(spot != 0)(start)
                else:
                    start()
            return carry

        lax.fori_loop(0, 8, step, 0)
        for i in range(8):
            if MOVES[i] == 0:
                dst[i * 8 + here] = src[here * 8 + plane(s * (4 - i))]

    def await_blocks(ref, sem):
        part = ref.at[pl.ds(0, REMOTE)]
        pltpu.make_async_copy(part, part, sem).wait()

    sums_copy.wait()
    total = sums_tx[...] + sums_rx[...]
    inverse = lax.rsqrt(total[0:1] / D + EPS)
    factor = inverse * inverse * inverse * total[1:2] / D
    inv[...] = jnp.broadcast_to(inverse, (128, TOK)).T
    coef[...] = jnp.broadcast_to(factor, (128, TOK)).T

    def finished(f):
        back = inv[...] * scaled[f] - emb[f].astype(F32) * coef[...]
        return (st[f].astype(F32) + back).astype(BF16)

    def swap(c):
        return pltpu.make_async_remote_copy(
            src_ref=rows_tx.at[c],
            dst_ref=rows_rx.at[c],
            send_sem=row_ssem.at[c],
            recv_sem=row_rsem.at[c],
            device_id={"pipe": 1 - core},
            device_id_type=MESH,
        )

    def hand_over(c):
        rows_tx[c] = finished((1 - core) * NC + c)
        swap(c).start()

    def direction(c):
        return 1 - 2 * (c % 2)

    def spread(c):
        def slots(i, rows):
            send[c, :, i * CAP : (i + 1) * CAP, :] = (
                jnp.dot(place[i], rows, preferred_element_type=F32).astype(BF16).reshape(NDP, CAP, CF)
            )

        slots(0, finished(core * NC + c))
        swap(c).wait()
        slots(1, rows_rx[c])
        send_blocks(send.at[c], recv.at[c], ssem.at[c], rsem.at[c], direction(c))

    def summed(c, first, groups):
        rows = recv[c, first * 8 : (first + groups) * 8].reshape(groups * GROUP, CF)
        picks = onehot[c % 2, :, first * GROUP : (first + groups) * GROUP]
        return jnp.dot(picks, rows, preferred_element_type=F32)

    def pass_on(src, dst, c, i, s):
        return pltpu.make_async_remote_copy(
            src_ref=src.at[c],
            dst_ref=dst.at[c],
            send_sem=tab_ssem.at[i, c],
            recv_sem=tab_rsem.at[i, c],
            device_id={"dp": here * 8 + plane(s)},
            device_id_type=MESH,
        )

    def far(c):
        return pass_on(far_tx, far_rx, c, 0, direction(c))

    def near(c):
        return pass_on(near_tx, near_rx, c, 1, direction(c))

    def back(c):
        return pass_on(back_tx, back_rx, c, 2, -direction(c))

    def first_sums(c):
        await_blocks(recv.at[c], rsem.at[c])
        far_tx[c] = summed(c, 0, 3).astype(BF16)
        far(c).start()
        back_tx[c] = summed(c, 5, 3).astype(BF16)
        back(c).start()

    def second_sums(c):
        own = summed(c, 3, 1)
        far(c).wait_recv()
        near_tx[c] = (own + far_rx[c].astype(F32)).astype(BF16)
        near(c).start()

    def last_sums(c):
        own = summed(c, 4, 1)
        back(c).wait_recv()
        own = own + back_rx[c].astype(F32)
        near(c).wait_recv()
        own = own + near_rx[c].astype(F32)
        table[:, :, c * CF : (c + 1) * CF] = own[:VR].reshape(VR, 1, CF)

    hand_over(0)
    hand_over(1)
    spread(0)
    for kind in range(2):
        send_blocks(isend, irecv.at[kind], issem.at[kind], irsem.at[kind], 1 - 2 * kind)
    for c in range(1, AHEAD):
        hand_over(c + 1)
        spread(c)

    slot = lax.broadcasted_iota(I32, (NDP, ROWS), 1)
    unfold = jnp.where(slot // (2 * CAP) == lax.broadcasted_iota(I32, (NDP, ROWS), 0), 1.0, 0.0).astype(BF16)
    lane = lax.broadcasted_iota(I32, (2 * CAP, ROWS), 1) % (2 * CAP)
    take = lane == lax.broadcasted_iota(I32, (2 * CAP, ROWS), 0)
    for kind in range(2):
        await_blocks(irecv.at[kind], irsem.at[kind])
        got = irecv[kind].reshape(NDP, 128).T[: 2 * CAP].astype(BF16)
        spots = jnp.dot(got, unfold, preferred_element_type=F32)
        index = jnp.sum(jnp.where(take, spots, 0.0), axis=0, keepdims=True).astype(I32) + HALF
        onehot[kind] = jnp.where(lax.broadcasted_iota(I32, (VP, ROWS), 0) == index, 1.0, 0.0).astype(BF16)

    for c in range(NC + 3):
        if c + AHEAD + 1 < NC:
            hand_over(c + AHEAD + 1)
        if c < NC:
            first_sums(c)
        if c + AHEAD < NC:
            spread(c + AHEAD)
        if 0 <= c - 2 < NC:
            second_sums(c - 2)
        if 0 <= c - 3 < NC:
            last_sums(c - 3)

    for kind in range(2):
        await_blocks(isend, issem.at[kind])
    for c in range(NC):
        await_blocks(send.at[c], ssem.at[c])
        for copy in (far(c), near(c), back(c)):
            copy.wait_send()


def on_device(token_ids, embedded, norm_gain, proj_grad, proj_weight, stream_grad):
    anywhere = pl.BlockSpec(memory_space=pl.ANY)
    vmem = pl.BlockSpec(memory_space=pltpu.VMEM)
    dma = pltpu.SemaphoreType.DMA
    table = pl.pallas_call(
        kernel,
        out_shape=pltpu.VMEM((VR, 1, FEAT // 2), F32),
        in_specs=[vmem, vmem] + [anywhere] * 4,
        out_specs=vmem,
        scratch_shapes=[
            pltpu.VMEM((TOK, INNER), BF16),
            pltpu.VMEM((NB, BF, INNER), BF16),
            pltpu.VMEM((NF, TOK, CF), BF16),
            pltpu.VMEM((NF, TOK, CF), BF16),
            pltpu.VMEM((NF, TOK, CF), F32),
            pltpu.VMEM((TOK, 128), F32),
            pltpu.VMEM((TOK, 128), F32),
            pltpu.VMEM((TOK, 128), F32),
            pltpu.VMEM((TOK, 128), F32),
            pltpu.VMEM((2, TOK), F32),
            pltpu.VMEM((2, TOK), F32),
            pltpu.VMEM((1, TOK), I32),
            pltpu.VMEM((2, SLOTS, TOK), BF16),
            pltpu.VMEM((NC, TOK, CF), BF16),
            pltpu.VMEM((NC, TOK, CF), BF16),
            pltpu.VMEM((NC, NDP, 2 * CAP, CF), BF16),
            pltpu.VMEM((NC, NDP, 2 * CAP, CF), BF16),
            pltpu.VMEM((NDP, 1, 128), F32),
            pltpu.VMEM((2, NDP, 1, 128), F32),
            pltpu.VMEM((2, VP, ROWS), BF16),
            pltpu.VMEM((NC, VP, CF), BF16),
            pltpu.VMEM((NC, VP, CF), BF16),
            pltpu.VMEM((NC, VP, CF), BF16),
            pltpu.VMEM((NC, VP, CF), BF16),
            pltpu.VMEM((NC, VP, CF), BF16),
            pltpu.VMEM((NC, VP, CF), BF16),
            dma((1 + NB + 2 * NF,)),
            dma((2,)),
            dma((2,)),
            dma((NC,)),
            dma((NC,)),
            dma((NC,)),
            dma((NC,)),
            dma((2,)),
            dma((2,)),
            dma((3, NC)),
            dma((3, NC)),
        ],
        compiler_params=pltpu.CompilerParams(
            collective_id=0, has_side_effects=True, vmem_limit_bytes=56 * 1024 * 1024
        ),
    )(
        token_ids,
        norm_gain.reshape(NB, 1, BF),
        embedded,
        proj_grad,
        proj_weight,
        stream_grad,
    )
    return table


def solution(mesh):
    return jax.shard_map(
        on_device,
        mesh=mesh,
        in_specs=(
            P("pipe", "dp"),
            P("pipe", "dp", "mp"),
            P("pipe", "mp"),
            P("pipe", "dp", None),
            P("pipe", "mp", None),
            P("pipe", "dp", "mp"),
        ),
        out_specs=P("dp", "mp", "pipe"),
        check_vma=False,
    )
```
